256 devices in a mesh: req: 2 (over y), blk: 16 (over z), uly: 8 (over x, core).
Axes of the slice: x: 4, y: 2, z: 16, core: 2. Of those that a mesh axis runs over, the one named last changes fastest.
The devices are a block of a 4x16x16 slice.
Arguments:
- video_qkv: bfloat16 [3, 16384, 3072], P(None, ('req', 'blk', 'uly')), parts along dimension 1, may hold values from -16 to 16
- text_qkv: bfloat16 [3, 512, 3072], P(None, ('req', 'blk', 'uly')), parts along dimension 1, may hold values from -9.5625 to 9.5625
- video_gate: float32 [6144], P('req'), parts along dimension 0, may hold values from 1 to 4
- text_gate: float32 [6144], P('req'), parts along dimension 0, may hold values from 1 to 4
Outputs:
- video_out: bfloat16 [16384, 3072], P(('req', 'blk', 'uly')), parts along dimension 0
- text_out: bfloat16 [512, 3072], P(('req', 'blk', 'uly')), parts along dimension 0
The draws below stay inside these ranges and needn't reach their ends.
There are 2 independent parts, one for each index of `req`. The reference program is written for one: setup_inputs(seed, part) draws one part's arguments, and reference() takes and returns one part's arrays. A program takes and returns all parts, laid end to end along the dimension named above; each array names one. Nothing has to cross between parts.
All inputs are finite; a program needn't handle non-finite values.
Results may differ from the reference program's by a relative error of at most 0.0085.
Values may be sent and summed in bfloat16 or wider, within the bound.
A program may use at most 128 MiB of HBM per device.

```python
import math
import jax
import jax.numpy as jnp
from jax import lax

HEADS = 24
HD = 128
D = 3072
TOKENS = 8192
TXT = 256


def draw_video_qkv(key, part):
    base = jnp.clip(jax.random.normal(key, (3, TOKENS, D), jnp.float32) * 1.6, -9.6, 9.6)
    return base.astype(jnp.bfloat16)


def level_of(own_key, shape, cuts, least, largest):
    level, own = 1.0, jax.random.fold_in(own_key, 6)
    for dim, parts in cuts:
        steps = jnp.exp(jax.random.uniform(jax.random.fold_in(own, dim), (parts,), jnp.float32, least / len(cuts), largest / len(cuts)))
        level = level * jnp.repeat(steps, shape[dim] // parts).reshape([-1 if axis == dim else 1 for axis in range(len(shape))])
    return level


def bell_draw(stream_key, dims, scale, bound, shards=(), dtype=jnp.bfloat16):
    factor_of = level_of(stream_key, dims, shards, -0.22, 0.18) if shards else 1.0
    entries = jax.random.normal(stream_key, dims, jnp.float32) * scale * factor_of
    return jnp.minimum(jnp.maximum(entries, -bound), bound).astype(dtype)


def setup_inputs(seed: int = 0, part: int = 0) -> dict:
    splits = jax.random.split(jax.random.key(seed), 5)
    part_splits = jax.random.split(jax.random.fold_in(splits[4], part), 5)
    return {
        "video_qkv": draw_video_qkv(jax.random.fold_in(jax.random.fold_in(splits[4], part), 71), part),
        "text_qkv": bell_draw(part_splits[1], (3, TXT, D), 1.6, 9.5625, ((1, 128),)),
        "video_gate": jnp.clip(jnp.exp(jax.random.uniform(part_splits[2], (D,), jnp.float32, math.log(1.0), math.log(4.0))), 1.0, 4.0),
        "text_gate": jnp.clip(jnp.exp(jax.random.uniform(part_splits[3], (D,), jnp.float32, math.log(1.0), math.log(4.0))), 1.0, 4.0),
    }


def one_head(operands):
    queries, keys, values = operands
    scores = jnp.dot(queries, keys.T, precision=lax.Precision.HIGHEST) / math.sqrt(HD)
    best = lax.optimization_barrier(jnp.max(scores, axis=1))
    raised = jnp.exp(scores - best[:, None])
    total = lax.optimization_barrier(jnp.sum(raised, axis=1))
    weights = lax.optimization_barrier(raised.astype(jnp.bfloat16)).astype(jnp.float32)
    return jnp.dot(weights, values, precision=lax.Precision.HIGHEST) / total[:, None]

def reference(video_qkv, text_qkv, video_gate, text_gate):
    joint = jnp.concatenate((video_qkv, text_qkv), axis=1).astype(jnp.float32)
    length = joint.shape[1]
    split = joint.reshape(3, length, HEADS, HD).transpose(0, 2, 1, 3)
    heads_out = lax.map(one_head, (split[0], split[1], split[2]))
    attended = heads_out.transpose(1, 0, 2).reshape(length, HEADS * HD).astype(jnp.bfloat16)
    attended = lax.optimization_barrier(attended).astype(jnp.float32)
    video_out = (attended[:TOKENS] * video_gate[None, :]).astype(jnp.bfloat16)
    text_out = (attended[TOKENS:] * text_gate[None, :]).astype(jnp.bfloat16)
    return (video_out, text_out)
```

```python
import functools
import math

import jax
import jax.numpy as jnp
from jax import lax
from jax.experimental import pallas as pl
from jax.experimental.pallas import tpu as pltpu
from jax.sharding import PartitionSpec as P

HD = 128
MESH = pl.DeviceIdType.MESH
TILES = 6
PER = 4


def near(j, n):
    return (j + 1) // 2 if j % 2 else (n - j // 2) % n


def tile_sources(nb):
    out = []
    for s in range(TILES):
        if s % 3 == 1:
            first = (s // 3) * PER
            offs = [2 * near(nb // 2 - 1 - first - i, nb // 2) for i in range(PER)]
            out.append((True, offs))
        else:
            first = (s - (s + 1) // 3) * PER
            offs = [near(nb - 1 - first - i, nb) for i in range(PER)]
            out.append((False, offs))
    return out


def kernel(
    nb, nu, vid, txt, vgate, tgate, vout, tout,
    st, stt, kvb, txb, qb, qtb, ob, otb, qf, qq, ktx, tf, m_sc, acc_sc,
    l_st, l_kv, l_q, zs_kv, zr_kv, zs_t, zr_t, zs_q, zr_q, zs_qt, zr_qt,
    xs, xl, xr, xf0, xf1, pc, ts, tr, os_, orv, ots, otr, ol,
):
    z = lax.axis_index("blk")
    u = lax.axis_index("uly")
    rows = vid.shape[1]
    trows = txt.shape[1]
    up = u + 1 - 2 * lax.rem(u, 2)
    ul = lax.rem(u + nu - 2, nu)
    ur = lax.rem(u + 2, nu)
    uf = lax.rem(u + 4, nu)

    barrier = pltpu.get_barrier_semaphore()
    for e in range(1, nb):
        pl.semaphore_signal(
            barrier, inc=1, device_id={"blk": lax.rem(z + e, nb)}, device_id_type=MESH
        )
    for e in range(1, nu):
        pl.semaphore_signal(
            barrier, inc=1, device_id={"uly": lax.rem(u + e, nu)}, device_id_type=MESH
        )

    def cols(h):
        return pl.ds(pl.multiple_of(h * HD, HD), HD)

    heads = st.shape[0]

    def stage(h, _):
        pltpu.make_async_copy(vid.at[:, :, cols(h)], st.at[h], l_st.at[0]).start()
        pltpu.make_async_copy(txt.at[:, :, cols(h)], stt.at[h], l_st.at[1]).start()
        return 0

    lax.fori_loop(0, heads, stage, 0)

    def low(t):
        return 3 * (t // 2) + lax.rem(t, 2)

    def own(t):
        return 3 * (t // 2) + 2 * lax.rem(t, 2)

    def shared(t):
        return 3 * (t // 2) + 1

    hs = low(z)
    for k in range(2):
        pltpu.make_async_copy(
            vid.at[pl.ds(1, 2), :, cols(hs + k)], kvb.at[u, 0, k], l_kv.at[k]
        ).start()
        pltpu.make_async_copy(
            txt.at[pl.ds(1, 2), :, cols(hs + k)], txb.at[u, 0, k], l_kv.at[2 + k]
        ).start()
    plan = tile_sources(nb)
    locals_q = []
    for s, (both, offs) in enumerate(plan):
        for i, d in enumerate(offs):
            if d == 0:
                h = shared(z) if both else own(z)
                a = pltpu.make_async_copy(vid.at[0, :, cols(h)], qb.at[s, i], l_q.at[2 * len(locals_q)])
                b = pltpu.make_async_copy(txt.at[0, :, cols(h)], qtb.at[s, i], l_q.at[2 * len(locals_q) + 1])
                a.start()
                b.start()
                locals_q.append((a, b))

    pltpu.make_async_copy(st, st, l_st.at[0]).wait()
    pltpu.make_async_copy(stt, stt, l_st.at[1]).wait()
    pl.semaphore_wait(barrier, nb - 1 + nu - 1)

    def send(src, dst, ss, rs, dev):
        pltpu.make_async_remote_copy(
            src_ref=src, dst_ref=dst, send_sem=ss, recv_sem=rs, device_id=dev, device_id_type=MESH
        ).start()

    for j in range(1, nb):
        d = near(j, nb)
        t = lax.rem(z + nb - d, nb)
        h = low(t)
        send(st.at[pl.ds(h, 2), pl.ds(1, 2)], kvb.at[u, d], zs_kv, zr_kv.at[d], {"blk": t})
        send(stt.at[pl.ds(h, 2), pl.ds(1, 2)], txb.at[u, d], zs_t, zr_t, {"blk": t})
    for s, (both, offs) in enumerate(plan):
        for i, d in enumerate(offs):
            if d == 0:
                continue
            t = lax.rem(z + nb - d, nb)
            h = shared(t) if both else own(t)
            send(st.at[h, 0], qb.at[s, i], zs_q, zr_q.at[s], {"blk": t})
            send(stt.at[h, 0], qtb.at[s, i], zs_qt, zr_qt.at[s], {"blk": t})

    def arrived(ref, sem):
        pltpu.make_async_copy(ref, ref, sem).wait()

    right, left, partner = {"uly": ur}, {"uly": ul}, {"uly": up}

    def own_piece(d):
        if d == 0:
            for k in range(2):
                arrived(kvb.at[u, 0, k], l_kv.at[k])
        else:
            arrived(kvb.at[u, d], zr_kv.at[d])
        piece = kvb.at[u, d]
        send(piece, piece, xs.at[0], xl.at[d], right)
        send(piece, piece, xs.at[1], xr.at[d], left)
        send(piece, piece, xs.at[2], pc, partner)

    def next_piece(d):
        arrived(kvb.at[ul, d], xl.at[d])
        send(kvb.at[ul, d, 0], kvb.at[ul, d, 0], xs.at[0], xf0.at[d], right)
        send(kvb.at[ul, d], kvb.at[ul, d], xs.at[2], pc, partner)
        arrived(kvb.at[ur, d], xr.at[d])
        send(kvb.at[ur, d, 1], kvb.at[ur, d, 1], xs.at[1], xf1.at[d], left)
        send(kvb.at[ur, d], kvb.at[ur, d], xs.at[2], pc, partner)

    def far_piece(d):
        arrived(kvb.at[uf, d, 0], xf0.at[d])
        send(kvb.at[uf, d, 0], kvb.at[uf, d, 0], xs.at[2], pc, partner)
        arrived(kvb.at[uf, d, 1], xf1.at[d])
        send(kvb.at[uf, d, 1], kvb.at[uf, d, 1], xs.at[2], pc, partner)

    for j in range(nb + 2):
        if j < nb:
            own_piece(near(j, nb))
        if j == nb - 1:
            for k in range(2):
                arrived(txb.at[u, 0, k], l_kv.at[2 + k])
            arrived(txb.at[u, pl.ds(1, nb - 1)], zr_t)
            for e in range(1, nu):
                send(txb.at[u], txb.at[u], ts, tr, {"uly": lax.rem(u + e, nu)})
        if 1 <= j <= nb:
            next_piece(near(j - 1, nb))
        if j >= 2:
            far_piece(near(j - 2, nb))
    arrived(txb.at[pl.ds(0, nu - 1)], tr)

    for k in range(2):
        for kv in range(2):
            for v in range(nu):
                for d in range(nb):
                    at = (v * nb + d) * trows
                    tf[at : at + trows, :] = txb[v, d, k, kv].astype(jnp.float32)
            ktx[k, kv] = tf[...].astype(jnp.bfloat16)
    arrived(kvb.at[pl.ds(0, nu // 2)], pc)

    scale = math.log2(math.e) / math.sqrt(HD)
    vrows = PER * rows
    par = lax.rem(z, 2)

    def update(keys, values):
        kk = jnp.concatenate((keys, keys), axis=1)
        scores = lax.dot_general(
            qq[...], kk, (((1,), (1,)), ((), ())), preferred_element_type=jnp.float32
        )
        old = m_sc[...]
        best = jnp.maximum(old, jnp.max(scores, axis=1, keepdims=True))
        m_sc[...] = best
        raised = jnp.exp2(scores - best[:, :1]).astype(jnp.bfloat16)
        factor = jnp.exp2(old - best)
        vv = jnp.concatenate((values, jnp.ones_like(values)), axis=1)
        product = jnp.dot(raised, vv, preferred_element_type=jnp.float32)
        acc_sc[:, :HD] = acc_sc[:, :HD] * factor + product[:, :HD]
        acc_sc[:, HD:] = acc_sc[:, HD:] * factor + product[:, HD:]

    count = 0
    for s, (both, offs) in enumerate(plan):
        remote = sum(d != 0 for d in offs)
        if remote < PER:
            a, b = locals_q[count]
            a.wait()
            b.wait()
            count += 1
        arrived(qb.at[s, pl.ds(0, remote)], zr_q.at[s])
        arrived(qtb.at[s, pl.ds(0, remote)], zr_qt.at[s])
        qf[0:vrows, :] = qb[s].astype(jnp.float32).reshape(vrows, HD)
        for i in range(PER):
            at = vrows + i * trows
            qf[at : at + trows, :] = qtb[s, i].astype(jnp.float32)
        scaled = qf[...] * scale
        high = scaled.astype(jnp.bfloat16)
        qq[:, :HD] = high
        qq[:, HD:] = (scaled - high.astype(jnp.float32)).astype(jnp.bfloat16)
        m_sc[...] = jnp.full(m_sc.shape, -jnp.inf, jnp.float32)
        acc_sc[...] = jnp.zeros(acc_sc.shape, jnp.float32)
        slot = par if not both else 1 - par

        def chunk(c, _):
            update(
                kvb[c, :, slot, 0].reshape(nb * rows, HD),
                kvb[c, :, slot, 1].reshape(nb * rows, HD),
            )
            return 0

        lax.fori_loop(0, nu, chunk, 0)
        update(ktx[slot, 0], ktx[slot, 1])

        h = shared(z) if both else own(z)
        attended = (acc_sc[:, :HD] / acc_sc[:, HD:]).astype(jnp.bfloat16).astype(jnp.float32)
        gated = attended[:vrows] * vgate[pl.ds(h, 1), :]
        ob[s] = gated.astype(jnp.bfloat16).reshape(PER, rows, HD)
        tgated = attended[vrows:] * tgate[pl.ds(h, 1), :]
        for i in range(PER):
            otb[s, i] = tgated[i * trows : (i + 1) * trows].astype(jnp.bfloat16)
        for i, d in enumerate(offs):
            if d == 0:
                pltpu.make_async_copy(ob.at[s, i], vout.at[:, cols(h)], ol.at[2 * (count - 1)]).start()
                pltpu.make_async_copy(otb.at[s, i], tout.at[:, cols(h)], ol.at[2 * (count - 1) + 1]).start()
            else:
                t = lax.rem(z + d, nb)
                send(ob.at[s, i], vout.at[:, cols(h)], os_, orv, {"blk": t})
                send(otb.at[s, i], tout.at[:, cols(h)], ots, otr, {"blk": t})

    for k in range(2):
        arrived(ob.at[0, 0], ol.at[2 * k])
        arrived(otb.at[0, 0], ol.at[2 * k + 1])
    n_out = nb - 1 + nb // 2 - 1
    some = kvb.at[0, pl.ds(0, n_out // 2), 0]
    small = txb.at[0, pl.ds(0, n_out // 2), 0]
    for sem in (os_, orv, zs_q):
        arrived(some, sem)
    for sem in (ots, otr, zs_qt):
        arrived(small, sem)
    arrived(kvb.at[0, pl.ds(0, nb - 1)], zs_kv)
    arrived(txb.at[0, pl.ds(0, nb - 1)], zs_t)
    arrived(kvb.at[pl.ds(0, 3), pl.ds(0, nb // 2)], xs.at[0])
    arrived(kvb.at[pl.ds(0, 3), pl.ds(0, nb // 2)], xs.at[1])
    arrived(kvb.at[pl.ds(0, nu // 2)], xs.at[2])
    arrived(txb.at[pl.ds(0, nu - 1)], ts)


def on_device(video_qkv, text_qkv, video_gate, text_gate):
    nb = lax.axis_size("blk")
    nu = lax.axis_size("uly")
    rows, width = video_qkv.shape[1:]
    trows = text_qkv.shape[1]
    heads = width // HD
    bf, f32 = jnp.bfloat16, jnp.float32
    tile = PER * (rows + trows)
    dma = pltpu.SemaphoreType.DMA
    hbm = pl.BlockSpec(memory_space=pl.ANY)
    vmem = pl.BlockSpec(memory_space=pltpu.VMEM)
    return pl.pallas_call(
        functools.partial(kernel, nb, nu),
        out_shape=(
            jax.ShapeDtypeStruct((rows, width), bf),
            jax.ShapeDtypeStruct((trows, width), bf),
        ),
        in_specs=[hbm, hbm, vmem, vmem],
        out_specs=(hbm, hbm),
        scratch_shapes=[
            pltpu.VMEM((heads, 3, rows, HD), bf),
            pltpu.VMEM((heads, 3, trows, HD), bf),
            pltpu.VMEM((nu, nb, 2, 2, rows, HD), bf),
            pltpu.VMEM((nu, nb, 2, 2, trows, HD), bf),
            pltpu.VMEM((TILES, PER, rows, HD), bf),
            pltpu.VMEM((TILES, PER, trows, HD), bf),
            pltpu.VMEM((TILES, PER, rows, HD), bf),
            pltpu.VMEM((TILES, PER, trows, HD), bf),
            pltpu.VMEM((tile, HD), f32),
            pltpu.VMEM((tile, 2 * HD), bf),
            pltpu.VMEM((2, 2, nu * nb * trows, HD), bf),
            pltpu.VMEM((nu * nb * trows, HD), f32),
            pltpu.VMEM((tile, HD), f32),
            pltpu.VMEM((tile, 2 * HD), f32),
            dma((2,)), dma((4,)), dma((4,)),
            dma(()), dma((nb,)), dma(()), dma(()), dma(()), dma((TILES,)), dma(()), dma((TILES,)),
            dma((3,)), dma((nb,)), dma((nb,)), dma((nb,)), dma((nb,)), dma(()),
            dma(()), dma(()),
            dma(()), dma(()), dma(()), dma(()), dma((4,)),
        ],
        compiler_params=pltpu.CompilerParams(
            collective_id=0, has_side_effects=True, vmem_limit_bytes=60 * 1024 * 1024
        ),
        name="joint_attention",
    )(video_qkv, text_qkv, video_gate.reshape(heads, HD), text_gate.reshape(heads, HD))


def solution(mesh):
    in_specs = (
        P(None, ("req", "blk", "uly"), None),
        P(None, ("req", "blk", "uly"), None),
        P("req"),
        P("req"),
    )
    out_specs = (P(("req", "blk", "uly"), None), P(("req", "blk", "uly"), None))
    return jax.shard_map(
        on_device, mesh=mesh, in_specs=in_specs, out_specs=out_specs, check_vma=False
    )
```

```python
import functools
import math

import jax
import jax.numpy as jnp
from jax import lax
from jax.experimental import pallas as pl
from jax.experimental.pallas import tpu as pltpu
from jax.sharding import PartitionSpec as P

HD = 128
MESH = pl.DeviceIdType.MESH
TILES = 3
LAG = 3


def near(j, n):
    if isinstance(j, int):
        return (j + 1) // 2 if j % 2 else (n - j // 2) % n
    return jnp.where(lax.rem(j, 2) == 1, (j + 1) // 2, lax.rem(n - j // 2, n))


def kernel(
    nb, nu, vid, txt, vgate, tgate, vout, tout,
    st, stt, kvb, txb, qb, qtb, ob, otb, qf, qq, ktx, tf, m_sc, acc_sc, s_a, s_b,
    l_st, l_kv, l_q, zs_kv, zr_kv, zs_t, zr_t, zs_q, zr_q, zs_qt, zr_qt,
    xs, xl, xr, xf0, xf1, pc, ts, tr, os_, orv, ots, otr, ol,
):
    z = lax.axis_index("blk")
    u = lax.axis_index("uly")
    rows = vid.shape[1]
    trows = txt.shape[1]
    per = nb // 2
    up = u + 1 - 2 * lax.rem(u, 2)
    ul = lax.rem(u + nu - 2, nu)
    ur = lax.rem(u + 2, nu)
    uf = lax.rem(u + 4, nu)
    par = lax.rem(z, 2)

    barrier = pltpu.get_barrier_semaphore()
    for e in range(1, nb):
        pl.semaphore_signal(
            barrier, inc=1, device_id={"blk": lax.rem(z + e, nb)}, device_id_type=MESH
        )
    for e in range(1, nu):
        pl.semaphore_signal(
            barrier, inc=1, device_id={"uly": lax.rem(u + e, nu)}, device_id_type=MESH
        )

    def cols(h):
        return pl.ds(pl.multiple_of(h * HD, HD), HD)

    heads = st.shape[0]

    def stage(h, _):
        pltpu.make_async_copy(vid.at[:, :, cols(h)], st.at[h], l_st.at[0]).start()
        pltpu.make_async_copy(txt.at[:, :, cols(h)], stt.at[h], l_st.at[1]).start()
        return 0

    lax.fori_loop(0, heads, stage, 0)

    def low(t):
        return 3 * (t // 2) + lax.rem(t, 2)

    def own(t):
        return 3 * (t // 2) + 2 * lax.rem(t, 2)

    def shared(t):
        return 3 * (t // 2) + 1

    def shared_to(e):
        up_to = lax.rem(z + e, nb)
        return jnp.where(lax.rem(up_to, 2) == 0, up_to, lax.rem(z + nb - e, nb))

    def shared_back(e):
        return lax.rem(z + nb + (2 * par - 1) * e, nb)

    hs = low(z)
    for k in range(2):
        pltpu.make_async_copy(
            vid.at[pl.ds(1, 2), :, cols(hs + k)], kvb.at[u, 0, k], l_kv.at[k]
        ).start()
        pltpu.make_async_copy(
            txt.at[pl.ds(1, 2), :, cols(hs + k)], txb.at[u, 0, k], l_kv.at[2 + k]
        ).start()
    for k, (s, h) in enumerate(((1, own(z)), (2, shared(z)))):
        pltpu.make_async_copy(vid.at[0, :, cols(h)], qb.at[s, per - 1], l_q.at[2 * k]).start()
        pltpu.make_async_copy(txt.at[0, :, cols(h)], qtb.at[s, per - 1], l_q.at[2 * k + 1]).start()

    pltpu.make_async_copy(st, st, l_st.at[0]).wait()
    pltpu.make_async_copy(stt, stt, l_st.at[1]).wait()
    pl.semaphore_wait(barrier, nb - 1 + nu - 1)

    def send(src, dst, ss, rs, dev):
        pltpu.make_async_remote_copy(
            src_ref=src, dst_ref=dst, send_sem=ss, recv_sem=rs, device_id=dev, device_id_type=MESH
        ).start()

    for s in range(TILES):
        for i in range(per):
            if s < 2:
                d = near(nb - 1 - per * s - i, nb)
                t = lax.rem(z + nb - d, nb)
                h = own(t)
            else:
                d = per - 1 - i
                t = shared_to(d)
                h = shared(t)
            if d != 0:
                send(st.at[h, 0], qb.at[s, i], zs_q, zr_q.at[s], {"blk": t})
                send(stt.at[h, 0], qtb.at[s, i], zs_qt, zr_qt.at[s], {"blk": t})
    for j in range(1, nb):
        d = near(j, nb)
        t = lax.rem(z + nb - d, nb)
        h = low(t)
        send(stt.at[pl.ds(h, 2), pl.ds(1, 2)], txb.at[u, d], zs_t, zr_t, {"blk": t})
    for j in range(1, nb):
        d = near(j, nb)
        t = lax.rem(z + nb - d, nb)
        h = low(t)
        send(st.at[pl.ds(h, 2), pl.ds(1, 2)], kvb.at[u, d], zs_kv, zr_kv.at[d], {"blk": t})

    def arrived(ref, sem):
        pltpu.make_async_copy(ref, ref, sem).wait()

    right, left, partner = {"uly": ur}, {"uly": ul}, {"uly": up}

    def pass_own(d):
        piece = kvb.at[u, d]
        send(piece, piece, xs.at[0], xl.at[d], right)
        send(piece, piece, xs.at[1], xr.at[d], left)
        send(piece, piece, xs.at[2], pc.at[d], partner)

    def own_piece(d):
        arrived(kvb.at[u, d], zr_kv.at[d])
        pass_own(d)

    def next_piece(d):
        arrived(kvb.at[ul, d], xl.at[d])
        send(kvb.at[ul, d, 0], kvb.at[ul, d, 0], xs.at[0], xf0.at[d], right)
        send(kvb.at[ul, d], kvb.at[ul, d], xs.at[2], pc.at[d], partner)
        arrived(kvb.at[ur, d], xr.at[d])
        send(kvb.at[ur, d, 1], kvb.at[ur, d, 1], xs.at[1], xf1.at[d], left)
        send(kvb.at[ur, d], kvb.at[ur, d], xs.at[2], pc.at[d], partner)

    def far_piece(d):
        arrived(kvb.at[uf, d, 0], xf0.at[d])
        send(kvb.at[uf, d, 0], kvb.at[uf, d, 0], xs.at[2], pc.at[d], partner)
        arrived(kvb.at[uf, d, 1], xf1.at[d])
        send(kvb.at[uf, d, 1], kvb.at[uf, d, 1], xs.at[2], pc.at[d], partner)

    scale = math.log2(math.e) / math.sqrt(HD)
    vrows = per * rows
    n_all = vrows + per * trows
    slots = (par, par, 1 - par)

    def scores_of(s, keys):
        kk = jnp.concatenate((keys, keys), axis=1)
        return lax.dot_general(
            qq[s], kk, (((1,), (1,)), ((), ())), preferred_element_type=jnp.float32
        )

    def soften(s, sref, values):
        scores = sref[...]
        old = m_sc[s]
        best = jnp.maximum(old, jnp.max(scores, axis=1, keepdims=True))
        m_sc[s] = best
        raised = jnp.exp2(scores - best[:, :1]).astype(jnp.bfloat16)
        factor = jnp.exp2(old - best)
        vv = jnp.concatenate((values, jnp.ones_like(values)), axis=1)
        product = jnp.dot(raised, vv, preferred_element_type=jnp.float32)
        acc_sc[s, :, :HD] = acc_sc[s, :, :HD] * factor + product[:, :HD]
        acc_sc[s, :, HD:] = acc_sc[s, :, HD:] * factor + product[:, HD:]

    def step(block, n):
        bufs = (s_a, s_b)
        for s in range(TILES + 1):
            if s < TILES:
                bufs[s % 2][:, :n] = scores_of(s, block(slots[s], 0))
            if s > 0:
                soften(s - 1, bufs[(s - 1) % 2].at[:, :n], block(slots[s - 1], 1))

    for k in range(2):
        arrived(kvb.at[u, 0, k], l_kv.at[k])
    pass_own(0)
    for j in range(1, LAG):
        own_piece(near(j, nb))
        next_piece(near(j - 1, nb))
        if j >= 2:
            far_piece(near(j - 2, nb))

    for k in range(2):
        arrived(txb.at[u, 0, k], l_kv.at[2 + k])
    arrived(txb.at[u, pl.ds(1, nb - 1)], zr_t)
    for e in range(1, nu):
        send(txb.at[u], txb.at[u], ts, tr, {"uly": lax.rem(u + e, nu)})

    for s in range(TILES):
        remote = per
        if s > 0:
            arrived(qb.at[s, per - 1], l_q.at[2 * (s - 1)])
            arrived(qtb.at[s, per - 1], l_q.at[2 * (s - 1) + 1])
            remote = per - 1
        arrived(qb.at[s, pl.ds(0, remote)], zr_q.at[s])
        arrived(qtb.at[s, pl.ds(0, remote)], zr_qt.at[s])
        qf[0:vrows, :] = qb[s].astype(jnp.float32).reshape(vrows, HD)
        for i in range(per):
            at = vrows + i * trows
            qf[at : at + trows, :] = qtb[s, i].astype(jnp.float32)
        scaled = qf[...] * scale
        high = scaled.astype(jnp.bfloat16)
        qq[s, :, :HD] = high
        qq[s, :, HD:] = (scaled - high.astype(jnp.float32)).astype(jnp.bfloat16)
    m_sc[...] = jnp.full(m_sc.shape, -jnp.inf, jnp.float32)
    acc_sc[...] = jnp.zeros(acc_sc.shape, jnp.float32)

    arrived(txb.at[pl.ds(0, nu - 1)], tr)
    for k in range(2):
        for kv in range(2):
            for v in range(nu):
                for d in range(nb):
                    at = (v * nb + d) * trows
                    tf[at : at + trows, :] = txb[v, d, k, kv].astype(jnp.float32)
            ktx[k, kv] = tf[...].astype(jnp.bfloat16)
    step(lambda slot, kv: ktx[slot, kv], nu * nb * trows)

    def turn(j, _):
        @pl.when(j < nb)
        def _():
            own_piece(near(j, nb))

        @pl.when(j < nb + 1)
        def _():
            next_piece(near(j - 1, nb))

        @pl.when(j < nb + 2)
        def _():
            far_piece(near(j - 2, nb))

        d = near(j - LAG, nb)
        arrived(kvb.at[pl.ds(0, nu // 2), 0], pc.at[d])
        step(lambda slot, kv: kvb[:, d, slot, kv].reshape(nu * rows, HD), nu * rows)
        return 0

    lax.fori_loop(LAG, nb + LAG, turn, 0)

    for s in range(TILES):
        h = own(z) if s < 2 else shared(z)
        attended = (acc_sc[s, :, :HD] / acc_sc[s, :, HD:]).astype(jnp.bfloat16).astype(jnp.float32)
        gated = attended[:vrows] * vgate[pl.ds(h, 1), :]
        ob[s] = gated.astype(jnp.bfloat16).reshape(per, rows, HD)
        tgated = attended[vrows:] * tgate[pl.ds(h, 1), :]
        for i in range(per):
            otb[s, i] = tgated[i * trows : (i + 1) * trows].astype(jnp.bfloat16)
        for i in range(per):
            if s < 2:
                d = near(nb - 1 - per * s - i, nb)
                t = lax.rem(z + d, nb)
            else:
                d = per - 1 - i
                t = shared_back(d)
            if d == 0:
                at = 2 * (s - 1)
                pltpu.make_async_copy(ob.at[s, i], vout.at[:, cols(h)], ol.at[at]).start()
                pltpu.make_async_copy(otb.at[s, i], tout.at[:, cols(h)], ol.at[at + 1]).start()
            else:
                send(ob.at[s, i], vout.at[:, cols(h)], os_, orv, {"blk": t})
                send(otb.at[s, i], tout.at[:, cols(h)], ots, otr, {"blk": t})

    for k in range(2):
        arrived(ob.at[0, 0], ol.at[2 * k])
        arrived(otb.at[0, 0], ol.at[2 * k + 1])
    n_out = nb - 1 + per - 1
    some = kvb.at[0, pl.ds(0, n_out // 2), 0]
    small = txb.at[0, pl.ds(0, n_out // 2), 0]
    for sem in (os_, orv, zs_q):
        arrived(some, sem)
    for sem in (ots, otr, zs_qt):
        arrived(small, sem)
    arrived(kvb.at[0, pl.ds(0, nb - 1)], zs_kv)
    arrived(txb.at[0, pl.ds(0, nb - 1)], zs_t)
    arrived(kvb.at[pl.ds(0, 3), pl.ds(0, nb // 2)], xs.at[0])
    arrived(kvb.at[pl.ds(0, 3), pl.ds(0, nb // 2)], xs.at[1])
    arrived(kvb.at[pl.ds(0, nu // 2)], xs.at[2])
    arrived(txb.at[pl.ds(0, nu - 1)], ts)


def on_device(video_qkv, text_qkv, video_gate, text_gate):
    nb = lax.axis_size("blk")
    nu = lax.axis_size("uly")
    rows, width = video_qkv.shape[1:]
    trows = text_qkv.shape[1]
    heads = width // HD
    bf, f32 = jnp.bfloat16, jnp.float32
    per = nb // 2
    tile = per * (rows + trows)
    dma = pltpu.SemaphoreType.DMA
    hbm = pl.BlockSpec(memory_space=pl.ANY)
    vmem = pl.BlockSpec(memory_space=pltpu.VMEM)
    return pl.pallas_call(
        functools.partial(kernel, nb, nu),
        out_shape=(
            jax.ShapeDtypeStruct((rows, width), bf),
            jax.ShapeDtypeStruct((trows, width), bf),
        ),
        in_specs=[hbm, hbm, vmem, vmem],
        out_specs=(hbm, hbm),
        scratch_shapes=[
            pltpu.VMEM((heads, 3, rows, HD), bf),
            pltpu.VMEM((heads, 3, trows, HD), bf),
            pltpu.VMEM((nu, nb, 2, 2, rows, HD), bf),
            pltpu.VMEM((nu, nb, 2, 2, trows, HD), bf),
            pltpu.VMEM((TILES, per, rows, HD), bf),
            pltpu.VMEM((TILES, per, trows, HD), bf),
            pltpu.VMEM((TILES, per, rows, HD), bf),
            pltpu.VMEM((TILES, per, trows, HD), bf),
            pltpu.VMEM((tile, HD), f32),
            pltpu.VMEM((TILES, tile, 2 * HD), bf),
            pltpu.VMEM((2, 2, nu * nb * trows, HD), bf),
            pltpu.VMEM((nu * nb * trows, HD), f32),
            pltpu.VMEM((TILES, tile, HD), f32),
            pltpu.VMEM((TILES, tile, 2 * HD), f32),
            pltpu.VMEM((tile, nu * rows), f32),
            pltpu.VMEM((tile, nu * rows), f32),
            dma((2,)), dma((4,)), dma((4,)),
            dma(()), dma((nb,)), dma(()), dma(()), dma(()), dma((TILES,)), dma(()), dma((TILES,)),
            dma((3,)), dma((nb,)), dma((nb,)), dma((nb,)), dma((nb,)), dma((nb,)),
            dma(()), dma(()),
            dma(()), dma(()), dma(()), dma(()), dma((4,)),
        ],
        compiler_params=pltpu.CompilerParams(
            collective_id=0, has_side_effects=True, vmem_limit_bytes=60 * 1024 * 1024
        ),
        name="joint_attention",
    )(video_qkv, text_qkv, video_gate.reshape(heads, HD), text_gate.reshape(heads, HD))


def solution(mesh):
    in_specs = (
        P(None, ("req", "blk", "uly"), None),
        P(None, ("req", "blk", "uly"), None),
        P("req"),
        P("req"),
    )
    out_specs = (P(("req", "blk", "uly"), None), P(("req", "blk", "uly"), None))
    return jax.shard_map(
        on_device, mesh=mesh, in_specs=in_specs, out_specs=out_specs, check_vma=False
    )
```

```python
import functools
import math

import jax
import jax.numpy as jnp
from jax import lax
from jax.experimental import pallas as pl
from jax.experimental.pallas import tpu as pltpu
from jax.sharding import PartitionSpec as P

HD = 128
MESH = pl.DeviceIdType.MESH
TILES = 3
LAG = 3
DEPTH = 2 * LAG + 2


def near(j, n):
    if isinstance(j, int):
        return (j + 1) // 2 if j % 2 else (n - j // 2) % n
    return jnp.where(lax.rem(j, 2) == 1, (j + 1) // 2, lax.rem(n - j // 2, n))


def kernel(
    nb, nu, vid, txt, vgate, tgate, vout, tout,
    st, stt, kvb, txb, qb, qtb, ob, otb, qf, qq, ktx, tf, m_sc, acc_sc, s_a, s_b,
    l_st, l_kv, l_q, zs_kv, zs_r, zr_kv, zs_t, zr_t, zs_q, zr_q, zs_qt, zr_qt,
    xs, xl, xr, xf0, xf1, pc, ts, tr, os_, orv, ots, otr, ol,
):
    z = lax.axis_index("blk")
    u = lax.axis_index("uly")
    rows = vid.shape[1]
    trows = txt.shape[1]
    per = nb // 2
    up = u + 1 - 2 * lax.rem(u, 2)
    ul = lax.rem(u + nu - 2, nu)
    ur = lax.rem(u + 2, nu)
    uf = lax.rem(u + 4, nu)
    par = lax.rem(z, 2)

    barrier = pltpu.get_barrier_semaphore()
    for e in range(1, nb):
        pl.semaphore_signal(
            barrier, inc=1, device_id={"blk": lax.rem(z + e, nb)}, device_id_type=MESH
        )
    for e in range(1, nu):
        pl.semaphore_signal(
            barrier, inc=1, device_id={"uly": lax.rem(u + e, nu)}, device_id_type=MESH
        )

    def cols(h):
        return pl.ds(pl.multiple_of(h * HD, HD), HD)

    heads = st.shape[0]

    def stage(h, _):
        pltpu.make_async_copy(vid.at[:, :, cols(h)], st.at[h], l_st.at[0]).start()
        pltpu.make_async_copy(txt.at[:, :, cols(h)], stt.at[h], l_st.at[1]).start()
        return 0

    lax.fori_loop(0, heads, stage, 0)

    def low(t):
        return 3 * (t // 2) + lax.rem(t, 2)

    def own(t):
        return 3 * (t // 2) + 2 * lax.rem(t, 2)

    def shared(t):
        return 3 * (t // 2) + 1

    def shared_to(e):
        up_to = lax.rem(z + e, nb)
        return jnp.where(lax.rem(up_to, 2) == 0, up_to, lax.rem(z + nb - e, nb))

    def shared_back(e):
        return lax.rem(z + nb + (2 * par - 1) * e, nb)

    hs = low(z)
    for k, h in enumerate((own(z), shared(z))):
        pltpu.make_async_copy(
            vid.at[pl.ds(1, 2), :, cols(h)], kvb.at[k, u, 0], zr_kv.at[k, 0]
        ).start()
        pltpu.make_async_copy(
            txt.at[pl.ds(1, 2), :, cols(hs + k)], txb.at[u, 0, k], l_kv.at[k]
        ).start()
    for k, (s, h) in enumerate(((1, own(z)), (2, shared(z)))):
        pltpu.make_async_copy(vid.at[0, :, cols(h)], qb.at[s, per - 1], l_q.at[2 * k]).start()
        pltpu.make_async_copy(txt.at[0, :, cols(h)], qtb.at[s, per - 1], l_q.at[2 * k + 1]).start()

    pltpu.make_async_copy(st, st, l_st.at[0]).wait()
    pltpu.make_async_copy(stt, stt, l_st.at[1]).wait()
    pl.semaphore_wait(barrier, nb - 1 + nu - 1)

    def send(src, dst, ss, rs, dev):
        pltpu.make_async_remote_copy(
            src_ref=src, dst_ref=dst, send_sem=ss, recv_sem=rs, device_id=dev, device_id_type=MESH
        ).start()

    def send_queries(s):
        for i in range(per):
            if s < 2:
                d = near(nb - 1 - per * s - i, nb)
                t = lax.rem(z + nb - d, nb)
                h = own(t)
            else:
                d = per - 1 - i
                t = shared_to(d)
                h = shared(t)
            if d != 0:
                send(st.at[h, 0], qb.at[s, i], zs_q, zr_q.at[s], {"blk": t})
                send(stt.at[h, 0], qtb.at[s, i], zs_qt, zr_qt.at[s], {"blk": t})

    def send_own(j):
        d = near(j, nb)
        t = lax.rem(z + nb - d, nb)
        send(st.at[own(t), pl.ds(1, 2)], kvb.at[0, u, d], zs_kv, zr_kv.at[0, d], {"blk": t})

    send_queries(0)
    send_queries(1)
    for j in range(1, nb):
        d = near(j, nb)
        t = lax.rem(z + nb - d, nb)
        h = low(t)
        send(stt.at[pl.ds(h, 2), pl.ds(1, 2)], txb.at[u, d], zs_t, zr_t, {"blk": t})
    for e in range(1, per):
        t = shared_to(e)
        send(st.at[shared(t), pl.ds(1, 2)], kvb.at[1, u, e], zs_kv, zr_kv.at[1, e], {"blk": t})
    for j in range(1, per + 1):
        send_own(j)

    def piece_of(q):
        r = q - 2 * per
        late = lax.rem(r + 2 * per, 2)
        slot = jnp.where(q < per, 1, jnp.where(q < 2 * per, 0, late))
        j = jnp.where(q < 2 * per, q - per, per + r // 2)
        idx = jnp.where(q < per, q, jnp.where(late * (r >= 0) == 1, per + r // 2, near(jnp.maximum(j, 0), nb)))
        return slot, idx

    def arrived(ref, sem):
        pltpu.make_async_copy(ref, ref, sem).wait()

    right, left, partner = {"uly": ur}, {"uly": ul}, {"uly": up}

    def own_piece(q):
        k, i = piece_of(q)
        piece = kvb.at[k, u, i]
        arrived(piece, zr_kv.at[k, i])
        send(piece, piece, xs.at[0], xl.at[k, i], right)
        send(piece, piece, xs.at[1], xr.at[k, i], left)
        send(piece, piece, xs.at[2], pc.at[k, i], partner)

    def hand_on(e):
        send(kvb.at[1, u, e], kvb.at[1, u, per + e], zs_r, zr_kv.at[1, per + e], {"blk": z + 1 - 2 * par})

    def next_piece(q):
        k, i = piece_of(q)
        arrived(kvb.at[k, ul, i], xl.at[k, i])
        send(kvb.at[k, ul, i, 0], kvb.at[k, ul, i, 0], xs.at[0], xf0.at[k, i], right)
        send(kvb.at[k, ul, i], kvb.at[k, ul, i], xs.at[2], pc.at[k, i], partner)
        arrived(kvb.at[k, ur, i], xr.at[k, i])
        send(kvb.at[k, ur, i, 1], kvb.at[k, ur, i, 1], xs.at[1], xf1.at[k, i], left)
        send(kvb.at[k, ur, i], kvb.at[k, ur, i], xs.at[2], pc.at[k, i], partner)

    def far_piece(q):
        k, i = piece_of(q)
        arrived(kvb.at[k, uf, i, 0], xf0.at[k, i])
        send(kvb.at[k, uf, i, 0], kvb.at[k, uf, i, 0], xs.at[2], pc.at[k, i], partner)
        arrived(kvb.at[k, uf, i, 1], xf1.at[k, i])
        send(kvb.at[k, uf, i, 1], kvb.at[k, uf, i, 1], xs.at[2], pc.at[k, i], partner)

    scale = math.log2(math.e) / math.sqrt(HD)
    vrows = per * rows
    n_all = vrows + per * trows
    slots = (par, par, 1 - par)

    def scores_of(s, keys):
        kk = jnp.concatenate((keys, keys), axis=1)
        return lax.dot_general(
            qq[s], kk, (((1,), (1,)), ((), ())), preferred_element_type=jnp.float32
        )

    def soften(s, sref, values):
        scores = sref[...]
        old = m_sc[s]
        best = jnp.maximum(old, jnp.max(scores, axis=1, keepdims=True))
        m_sc[s] = best
        raised = jnp.exp2(scores - best[:, :1]).astype(jnp.bfloat16)
        factor = jnp.exp2(old - best)
        vv = jnp.concatenate((values, jnp.ones_like(values)), axis=1)
        product = jnp.dot(raised, vv, preferred_element_type=jnp.float32)
        acc_sc[s, :, :HD] = acc_sc[s, :, :HD] * factor + product[:, :HD]
        acc_sc[s, :, HD:] = acc_sc[s, :, HD:] * factor + product[:, HD:]

    bufs = (s_a, s_b)

    def step(block, n):
        for s in range(3):
            if s < 2:
                bufs[s % 2][:, :n] = scores_of(s, block(slots[s], 0))
            if s > 0:
                soften(s - 1, bufs[(s - 1) % 2].at[:, :n], block(slots[s - 1], 1))

    def prepare(s):
        remote = per
        if s > 0:
            arrived(qb.at[s, per - 1], l_q.at[2 * (s - 1)])
            arrived(qtb.at[s, per - 1], l_q.at[2 * (s - 1) + 1])
            remote = per - 1
        arrived(qb.at[s, pl.ds(0, remote)], zr_q.at[s])
        arrived(qtb.at[s, pl.ds(0, remote)], zr_qt.at[s])
        qf[0:vrows, :] = qb[s].astype(jnp.float32).reshape(vrows, HD)
        for i in range(per):
            at = vrows + i * trows
            qf[at : at + trows, :] = qtb[s, i].astype(jnp.float32)
        scaled = qf[...] * scale
        high = scaled.astype(jnp.bfloat16)
        qq[s, :, :HD] = high
        qq[s, :, HD:] = (scaled - high.astype(jnp.float32)).astype(jnp.bfloat16)

    def finish(s):
        h = own(z) if s < 2 else shared(z)
        attended = (acc_sc[s, :, :HD] / acc_sc[s, :, HD:]).astype(jnp.bfloat16).astype(jnp.float32)
        gated = attended[:vrows] * vgate[pl.ds(h, 1), :]
        ob[s] = gated.astype(jnp.bfloat16).reshape(per, rows, HD)
        tgated = attended[vrows:] * tgate[pl.ds(h, 1), :]
        for i in range(per):
            otb[s, i] = tgated[i * trows : (i + 1) * trows].astype(jnp.bfloat16)
        for i in range(per):
            if s < 2:
                d = near(nb - 1 - per * s - i, nb)
                t = lax.rem(z + d, nb)
            else:
                d = per - 1 - i
                t = shared_back(d)
            if d == 0:
                at = 2 * (s - 1)
                pltpu.make_async_copy(ob.at[s, i], vout.at[:, cols(h)], ol.at[at]).start()
                pltpu.make_async_copy(otb.at[s, i], tout.at[:, cols(h)], ol.at[at + 1]).start()
            else:
                send(ob.at[s, i], vout.at[:, cols(h)], os_, orv, {"blk": t})
                send(otb.at[s, i], tout.at[:, cols(h)], ots, otr, {"blk": t})

    def carry(q):
        @pl.when(q < 2 * nb)
        def _():
            own_piece(q)

        @pl.when(q < per)
        def _():
            hand_on(q)

        @pl.when((q >= 1) & (q < per))
        def _():
            send_own(per + q)

        @pl.when((q >= LAG) & (q < 2 * nb + LAG))
        def _():
            next_piece(q - LAG)

        @pl.when((q >= 2 * LAG) & (q < 2 * nb + 2 * LAG))
        def _():
            far_piece(q - 2 * LAG)

    def early(q, _):
        carry(q)
        return 0

    lax.fori_loop(0, per, early, 0)
    send_queries(2)

    for k in range(2):
        arrived(txb.at[u, 0, k], l_kv.at[k])
    arrived(txb.at[u, pl.ds(1, nb - 1)], zr_t)
    for e in range(1, nu):
        send(txb.at[u], txb.at[u], ts, tr, {"uly": lax.rem(u + e, nu)})
    m_sc[...] = jnp.full(m_sc.shape, -jnp.inf, jnp.float32)
    acc_sc[...] = jnp.zeros(acc_sc.shape, jnp.float32)
    prepare(0)
    prepare(1)
    lax.fori_loop(per, per + LAG, early, 0)

    arrived(txb.at[pl.ds(0, nu - 1)], tr)
    for k in range(2):
        for kv in range(2):
            for v in range(nu):
                for d in range(nb):
                    at = (v * nb + d) * trows
                    tf[at : at + trows, :] = txb[v, d, k, kv].astype(jnp.float32)
            ktx[k, kv] = tf[...].astype(jnp.bfloat16)
    step(lambda slot, kv: ktx[slot, kv], nu * nb * trows)

    quarter = kvb.at[0, pl.ds(0, nu // 2), 0]

    def turn(q, _):
        carry(q)
        r = q - DEPTH

        @pl.when((r >= per) & ((r < 2 * per) | (lax.rem(r + DEPTH, 2) == 0)))
        def _():
            k, d = piece_of(r)
            arrived(quarter, pc.at[0, d])
            step(lambda slot, kv: kvb[0, :, d, kv].reshape(nu * rows, HD), nu * rows)

        return 0

    lax.fori_loop(per + LAG, 2 * nb + DEPTH - 1, turn, 0)
    finish(0)
    finish(1)

    prepare(2)
    n = nu * nb * trows

    def shared_block(b, kv):
        return kvb[1, :, b, kv].reshape(nu * rows, HD)

    arrived(quarter, pc.at[1, 0])
    s_a[...] = scores_of(2, shared_block(0, 0))

    def pair(i, _):
        b = 2 * i
        arrived(quarter, pc.at[1, b + 1])
        s_b[...] = scores_of(2, shared_block(b + 1, 0))
        soften(2, s_a, shared_block(b, 1))

        @pl.when(b + 2 < nb)
        def _():
            arrived(quarter, pc.at[1, b + 2])

        s_a[...] = scores_of(2, shared_block(lax.rem(b + 2, nb), 0))
        soften(2, s_b, shared_block(b + 1, 1))
        return 0

    lax.fori_loop(0, per, pair, 0)
    s_b[:, :n] = scores_of(2, ktx[slots[2], 0])
    soften(2, s_b.at[:, :n], ktx[slots[2], 1])
    finish(2)

    for k in range(2):
        arrived(ob.at[0, 0], ol.at[2 * k])
        arrived(otb.at[0, 0], ol.at[2 * k + 1])
    n_out = nb - 1 + per - 1
    some = kvb.at[0, 0, pl.ds(0, n_out // 2)]
    small = txb.at[0, pl.ds(0, n_out // 2), 0]
    for sem in (os_, orv, zs_q):
        arrived(some, sem)
    for sem in (ots, otr, zs_qt):
        arrived(small, sem)
    arrived(kvb.at[0, pl.ds(0, 2), pl.ds(0, n_out // 2)], zs_kv)
    arrived(kvb.at[0, 0, pl.ds(0, per)], zs_r)
    arrived(txb.at[0, pl.ds(0, nb - 1)], zs_t)
    arrived(kvb.at[0, pl.ds(0, 3)], xs.at[0])
    arrived(kvb.at[0, pl.ds(0, 3)], xs.at[1])
    arrived(kvb.at[0], xs.at[2])
    arrived(txb.at[pl.ds(0, nu - 1)], ts)


def on_device(video_qkv, text_qkv, video_gate, text_gate):
    nb = lax.axis_size("blk")
    nu = lax.axis_size("uly")
    rows, width = video_qkv.shape[1:]
    trows = text_qkv.shape[1]
    heads = width // HD
    bf, f32 = jnp.bfloat16, jnp.float32
    per = nb // 2
    tile = per * (rows + trows)
    dma = pltpu.SemaphoreType.DMA
    hbm = pl.BlockSpec(memory_space=pl.ANY)
    vmem = pl.BlockSpec(memory_space=pltpu.VMEM)
    return pl.pallas_call(
        functools.partial(kernel, nb, nu),
        out_shape=(
            jax.ShapeDtypeStruct((rows, width), bf),
            jax.ShapeDtypeStruct((trows, width), bf),
        ),
        in_specs=[hbm, hbm, vmem, vmem],
        out_specs=(hbm, hbm),
        scratch_shapes=[
            pltpu.VMEM((heads, 3, rows, HD), bf),
            pltpu.VMEM((heads, 3, trows, HD), bf),
            pltpu.VMEM((2, nu, nb, 2, rows, HD), bf),
            pltpu.VMEM((nu, nb, 2, 2, trows, HD), bf),
            pltpu.VMEM((TILES, per, rows, HD), bf),
            pltpu.VMEM((TILES, per, trows, HD), bf),
            pltpu.VMEM((TILES, per, rows, HD), bf),
            pltpu.VMEM((TILES, per, trows, HD), bf),
            pltpu.VMEM((tile, HD), f32),
            pltpu.VMEM((TILES, tile, 2 * HD), bf),
            pltpu.VMEM((2, 2, nu * nb * trows, HD), bf),
            pltpu.VMEM((nu * nb * trows, HD), f32),
            pltpu.VMEM((TILES, tile, HD), f32),
            pltpu.VMEM((TILES, tile, 2 * HD), f32),
            pltpu.VMEM((tile, nu * rows), f32),
            pltpu.VMEM((tile, nu * rows), f32),
            dma((2,)), dma((2,)), dma((4,)),
            dma(()), dma(()), dma((2, nb)), dma(()), dma(()), dma(()), dma((TILES,)), dma(()), dma((TILES,)),
            dma((3,)), dma((2, nb)), dma((2, nb)), dma((2, nb)), dma((2, nb)), dma((2, nb)),
            dma(()), dma(()),
            dma(()), dma(()), dma(()), dma(()), dma((4,)),
        ],
        compiler_params=pltpu.CompilerParams(
            collective_id=0, has_side_effects=True, vmem_limit_bytes=60 * 1024 * 1024
        ),
        name="joint_attention",
    )(video_qkv, text_qkv, video_gate.reshape(heads, HD), text_gate.reshape(heads, HD))


def solution(mesh):
    in_specs = (
        P(None, ("req", "blk", "uly"), None),
        P(None, ("req", "blk", "uly"), None),
        P("req"),
        P("req"),
    )
    out_specs = (P(("req", "blk", "uly"), None), P(("req", "blk", "uly"), None))
    return jax.shard_map(
        on_device, mesh=mesh, in_specs=in_specs, out_specs=out_specs, check_vma=False
    )
```

```python
import functools
import math

import jax
import jax.numpy as jnp
from jax import lax
from jax.experimental import pallas as pl
from jax.experimental.pallas import tpu as pltpu
from jax.sharding import PartitionSpec as P

HD = 128
MESH = pl.DeviceIdType.MESH
TILES = 3
LAG = 3
DEPTH = 2 * LAG + 2


def near(j, n):
    if isinstance(j, int):
        return (j + 1) // 2 if j % 2 else (n - j // 2) % n
    return jnp.where(lax.rem(j, 2) == 1, (j + 1) // 2, lax.rem(n - j // 2, n))


def kernel(
    nb, nu, vid, txt, vgate, tgate, vout, tout,
    st, stt, kvb, txb, qb, qtb, ob, otb, qf, qq, ktx, tf, m_sc, acc_sc, s_a, s_b,
    l_st, l_kv, l_q, zs_kv, zs_r, zr_kv, zs_t, zr_t, zs_q, zr_q, zs_qt, zr_qt,
    xs, xl, xr, xf0, xf1, pc, ts, tr, os_, orv, ots, otr, ol,
):
    z = lax.axis_index("blk")
    u = lax.axis_index("uly")
    rows = vid.shape[1]
    trows = txt.shape[1]
    per = nb // 2
    up = u + 1 - 2 * lax.rem(u, 2)
    ul = lax.rem(u + nu - 2, nu)
    ur = lax.rem(u + 2, nu)
    uf = lax.rem(u + 4, nu)
    par = lax.rem(z, 2)

    barrier = pltpu.get_barrier_semaphore()
    for e in range(1, nb):
        pl.semaphore_signal(
            barrier, inc=1, device_id={"blk": lax.rem(z + e, nb)}, device_id_type=MESH
        )
    for e in range(1, nu):
        pl.semaphore_signal(
            barrier, inc=1, device_id={"uly": lax.rem(u + e, nu)}, device_id_type=MESH
        )

    def cols(h):
        return pl.ds(pl.multiple_of(h * HD, HD), HD)

    heads = st.shape[0]

    def stage(h, _):
        pltpu.make_async_copy(vid.at[:, :, cols(h)], st.at[h], l_st.at[0]).start()
        pltpu.make_async_copy(txt.at[:, :, cols(h)], stt.at[h], l_st.at[1]).start()
        return 0

    lax.fori_loop(0, heads, stage, 0)

    def low(t):
        return 3 * (t // 2) + lax.rem(t, 2)

    def own(t):
        return 3 * (t // 2) + 2 * lax.rem(t, 2)

    def shared(t):
        return 3 * (t // 2) + 1

    def shared_to(e):
        up_to = lax.rem(z + e, nb)
        return jnp.where(lax.rem(up_to, 2) == 0, up_to, lax.rem(z + nb - e, nb))

    def shared_back(e):
        return lax.rem(z + nb + (2 * par - 1) * e, nb)

    hs = low(z)
    for k, h in enumerate((own(z), shared(z))):
        pltpu.make_async_copy(
            vid.at[pl.ds(1, 2), :, cols(h)], kvb.at[k, u, 0], zr_kv.at[k, 0]
        ).start()
        pltpu.make_async_copy(
            txt.at[pl.ds(1, 2), :, cols(hs + k)], txb.at[u, 0, k], l_kv.at[k]
        ).start()
    for k, (s, h) in enumerate(((1, own(z)), (2, shared(z)))):
        pltpu.make_async_copy(vid.at[0, :, cols(h)], qb.at[s, per - 1], l_q.at[2 * k]).start()
        pltpu.make_async_copy(txt.at[0, :, cols(h)], qtb.at[s, per - 1], l_q.at[2 * k + 1]).start()

    pltpu.make_async_copy(st, st, l_st.at[0]).wait()
    pltpu.make_async_copy(stt, stt, l_st.at[1]).wait()
    pl.semaphore_wait(barrier, nb - 1 + nu - 1)

    def send(src, dst, ss, rs, dev):
        pltpu.make_async_remote_copy(
            src_ref=src, dst_ref=dst, send_sem=ss, recv_sem=rs, device_id=dev, device_id_type=MESH
        ).start()

    def send_queries(s):
        for i in range(per):
            if s < 2:
                d = near(nb - 1 - per * s - i, nb)
                t = lax.rem(z + nb - d, nb)
                h = own(t)
            else:
                d = per - 1 - i
                t = shared_to(d)
                h = shared(t)
            if d != 0:
                send(st.at[h, 0], qb.at[s, i], zs_q, zr_q.at[s], {"blk": t})
                send(stt.at[h, 0], qtb.at[s, i], zs_qt, zr_qt.at[s], {"blk": t})

    def send_own(j):
        d = near(j, nb)
        t = lax.rem(z + nb - d, nb)
        send(st.at[own(t), pl.ds(1, 2)], kvb.at[0, u, j], zs_kv, zr_kv.at[0, j], {"blk": t})

    send_queries(0)
    send_queries(1)
    for j in range(1, nb):
        d = near(j, nb)
        t = lax.rem(z + nb - d, nb)
        h = low(t)
        send(stt.at[pl.ds(h, 2), pl.ds(1, 2)], txb.at[u, d], zs_t, zr_t, {"blk": t})
    for e in range(1, per):
        t = shared_to(e)
        send(st.at[shared(t), pl.ds(1, 2)], kvb.at[1, u, e], zs_kv, zr_kv.at[1, e], {"blk": t})
    for j in range(1, per + 1):
        send_own(j)

    def piece_of(q):
        late = lax.rem(q, 2)
        slot = jnp.where(q < per, 1, jnp.where(q < 2 * per, 0, late))
        idx = jnp.where(q < per, q, jnp.where(q < 2 * per, q - per, q // 2))
        return slot, idx

    def arrived(ref, sem):
        pltpu.make_async_copy(ref, ref, sem).wait()

    right, left, partner = {"uly": ur}, {"uly": ul}, {"uly": up}

    def own_piece(q):
        k, i = piece_of(q)
        piece = kvb.at[k, u, i]
        arrived(piece, zr_kv.at[k, i])
        send(piece, piece, xs.at[0], xl.at[k, i], right)
        send(piece, piece, xs.at[1], xr.at[k, i], left)
        send(piece, piece, xs.at[2], pc.at[k, i], partner)

    def hand_on(e):
        send(kvb.at[1, u, e], kvb.at[1, u, per + e], zs_r, zr_kv.at[1, per + e], {"blk": z + 1 - 2 * par})

    def next_piece(q):
        k, i = piece_of(q)
        arrived(kvb.at[k, ul, i], xl.at[k, i])
        send(kvb.at[k, ul, i, 0], kvb.at[k, ul, i, 0], xs.at[0], xf0.at[k, i], right)
        send(kvb.at[k, ul, i], kvb.at[k, ul, i], xs.at[2], pc.at[k, i], partner)
        arrived(kvb.at[k, ur, i], xr.at[k, i])
        send(kvb.at[k, ur, i, 1], kvb.at[k, ur, i, 1], xs.at[1], xf1.at[k, i], left)
        send(kvb.at[k, ur, i], kvb.at[k, ur, i], xs.at[2], pc.at[k, i], partner)

    def far_piece(q):
        k, i = piece_of(q)
        arrived(kvb.at[k, uf, i, 0], xf0.at[k, i])
        send(kvb.at[k, uf, i, 0], kvb.at[k, uf, i, 0], xs.at[2], pc.at[k, i], partner)
        arrived(kvb.at[k, uf, i, 1], xf1.at[k, i])
        send(kvb.at[k, uf, i, 1], kvb.at[k, uf, i, 1], xs.at[2], pc.at[k, i], partner)

    scale = math.log2(math.e) / math.sqrt(HD)
    vrows = per * rows
    n_all = vrows + per * trows
    slots = (par, par, 1 - par)

    def scores_of(s, keys):
        kk = jnp.concatenate((keys, keys), axis=1)
        return lax.dot_general(
            qq[s], kk, (((1,), (1,)), ((), ())), preferred_element_type=jnp.float32
        )

    def soften(s, sref, values):
        scores = sref[...]
        old = m_sc[s]
        best = jnp.maximum(old, jnp.max(scores, axis=1, keepdims=True))
        m_sc[s] = best
        raised = jnp.exp2(scores - best[:, :1]).astype(jnp.bfloat16)
        factor = jnp.exp2(old - best)
        vv = jnp.concatenate((values, jnp.ones_like(values)), axis=1)
        product = jnp.dot(raised, vv, preferred_element_type=jnp.float32)
        acc_sc[s, :, :HD] = acc_sc[s, :, :HD] * factor + product[:, :HD]
        acc_sc[s, :, HD:] = acc_sc[s, :, HD:] * factor + product[:, HD:]

    bufs = (s_a, s_b)

    def step(block, n):
        for s in range(3):
            if s < 2:
                bufs[s % 2][:, :n] = scores_of(s, block(slots[s], 0))
            if s > 0:
                soften(s - 1, bufs[(s - 1) % 2].at[:, :n], block(slots[s - 1], 1))

    def prepare(s):
        remote = per
        if s > 0:
            arrived(qb.at[s, per - 1], l_q.at[2 * (s - 1)])
            arrived(qtb.at[s, per - 1], l_q.at[2 * (s - 1) + 1])
            remote = per - 1
        arrived(qb.at[s, pl.ds(0, remote)], zr_q.at[s])
        arrived(qtb.at[s, pl.ds(0, remote)], zr_qt.at[s])
        qf[0:vrows, :] = qb[s].astype(jnp.float32).reshape(vrows, HD)
        for i in range(per):
            at = vrows + i * trows
            qf[at : at + trows, :] = qtb[s, i].astype(jnp.float32)
        scaled = qf[...] * scale
        high = scaled.astype(jnp.bfloat16)
        qq[s, :, :HD] = high
        qq[s, :, HD:] = (scaled - high.astype(jnp.float32)).astype(jnp.bfloat16)

    def finish(s):
        h = own(z) if s < 2 else shared(z)
        attended = (acc_sc[s, :, :HD] / acc_sc[s, :, HD:]).astype(jnp.bfloat16).astype(jnp.float32)
        gated = attended[:vrows] * vgate[pl.ds(h, 1), :]
        ob[s] = gated.astype(jnp.bfloat16).reshape(per, rows, HD)
        tgated = attended[vrows:] * tgate[pl.ds(h, 1), :]
        for i in range(per):
            otb[s, i] = tgated[i * trows : (i + 1) * trows].astype(jnp.bfloat16)
        for i in range(per):
            if s < 2:
                d = near(nb - 1 - per * s - i, nb)
                t = lax.rem(z + d, nb)
            else:
                d = per - 1 - i
                t = shared_back(d)
            if d == 0:
                at = 2 * (s - 1)
                pltpu.make_async_copy(ob.at[s, i], vout.at[:, cols(h)], ol.at[at]).start()
                pltpu.make_async_copy(otb.at[s, i], tout.at[:, cols(h)], ol.at[at + 1]).start()
            else:
                send(ob.at[s, i], vout.at[:, cols(h)], os_, orv, {"blk": t})
                send(otb.at[s, i], tout.at[:, cols(h)], ots, otr, {"blk": t})

    def carry(q):
        @pl.when(q < 2 * nb)
        def _():
            own_piece(q)

        @pl.when(q < per)
        def _():
            hand_on(q)

        @pl.when((q >= 1) & (q < per))
        def _():
            send_own(per + q)

        @pl.when((q >= LAG) & (q < 2 * nb + LAG))
        def _():
            next_piece(q - LAG)

        @pl.when((q >= 2 * LAG) & (q < 2 * nb + 2 * LAG))
        def _():
            far_piece(q - 2 * LAG)

    def early(q, _):
        carry(q)
        return 0

    lax.fori_loop(0, per, early, 0)
    send_queries(2)

    for k in range(2):
        arrived(txb.at[u, 0, k], l_kv.at[k])
    arrived(txb.at[u, pl.ds(1, nb - 1)], zr_t)
    for e in range(1, nu):
        send(txb.at[u], txb.at[u], ts, tr, {"uly": lax.rem(u + e, nu)})
    m_sc[...] = jnp.full(m_sc.shape, -jnp.inf, jnp.float32)
    acc_sc[...] = jnp.zeros(acc_sc.shape, jnp.float32)
    prepare(0)
    prepare(1)
    lax.fori_loop(per, per + LAG, early, 0)

    arrived(txb.at[pl.ds(0, nu - 1)], tr)
    for k in range(2):
        for kv in range(2):
            for v in range(nu):
                for d in range(nb):
                    at = (v * nb + d) * trows
                    tf[at : at + trows, :] = txb[v, d, k, kv].astype(jnp.float32)
            ktx[k, kv] = tf[...].astype(jnp.bfloat16)
    step(lambda slot, kv: ktx[slot, kv], nu * nb * trows)

    quarter = kvb.at[0, pl.ds(0, nu // 2), 0]
    wide = 2 * nu * rows

    def keys_in(k, p):
        arrived(quarter, pc.at[k, 2 * p])
        arrived(quarter, pc.at[k, 2 * p + 1])

    def block(k, p, kv):
        return kvb[k, :, pl.ds(2 * p, 2), kv].reshape(wide, HD)

    def turn(q, _):
        carry(q)
        r = q - DEPTH
        place = lax.rem(r, 4)

        @pl.when(r == 2 * per)
        def _():
            prepare(2)

        @pl.when(((r > per) & (r < 2 * per) & (lax.rem(r, 2) == 1)) | ((r > 2 * per) & (place == 2)))
        def _():
            p = jnp.where(r < 2 * per, (r - per) // 2, r // 4)
            keys_in(0, p)
            step(lambda slot, kv: block(0, p, kv), wide)

        @pl.when((r >= 2 * per) & (place == 0))
        def _():
            p = r // 4 - per // 2
            keys_in(1, p)
            s_a[...] = scores_of(2, block(1, p, 0))
            soften(2, s_a, block(1, p, 1))

        return 0

    lax.fori_loop(per + LAG, 2 * nb + DEPTH - 1, turn, 0)
    finish(0)
    finish(1)

    n = nu * nb * trows
    bufs[0][:, :n] = scores_of(2, ktx[slots[2], 0])
    for i in range(per // 2):
        p = per // 2 + i
        keys_in(1, p)
        bufs[(i + 1) % 2][...] = scores_of(2, block(1, p, 0))
        if i == 0:
            soften(2, bufs[0].at[:, :n], ktx[slots[2], 1])
        else:
            soften(2, bufs[i % 2], block(1, p - 1, 1))
    soften(2, bufs[(per // 2) % 2], block(1, per - 1, 1))
    finish(2)

    for k in range(2):
        arrived(ob.at[0, 0], ol.at[2 * k])
        arrived(otb.at[0, 0], ol.at[2 * k + 1])
    n_out = nb - 1 + per - 1
    some = kvb.at[0, 0, pl.ds(0, n_out // 2)]
    small = txb.at[0, pl.ds(0, n_out // 2), 0]
    for sem in (os_, orv, zs_q):
        arrived(some, sem)
    for sem in (ots, otr, zs_qt):
        arrived(small, sem)
    arrived(kvb.at[0, pl.ds(0, 2), pl.ds(0, n_out // 2)], zs_kv)
    arrived(kvb.at[0, 0, pl.ds(0, per)], zs_r)
    arrived(txb.at[0, pl.ds(0, nb - 1)], zs_t)
    arrived(kvb.at[0, pl.ds(0, 3)], xs.at[0])
    arrived(kvb.at[0, pl.ds(0, 3)], xs.at[1])
    arrived(kvb.at[0], xs.at[2])
    arrived(txb.at[pl.ds(0, nu - 1)], ts)


def on_device(video_qkv, text_qkv, video_gate, text_gate):
    nb = lax.axis_size("blk")
    nu = lax.axis_size("uly")
    rows, width = video_qkv.shape[1:]
    trows = text_qkv.shape[1]
    heads = width // HD
    bf, f32 = jnp.bfloat16, jnp.float32
    per = nb // 2
    tile = per * (rows + trows)
    dma = pltpu.SemaphoreType.DMA
    hbm = pl.BlockSpec(memory_space=pl.ANY)
    vmem = pl.BlockSpec(memory_space=pltpu.VMEM)
    return pl.pallas_call(
        functools.partial(kernel, nb, nu),
        out_shape=(
            jax.ShapeDtypeStruct((rows, width), bf),
            jax.ShapeDtypeStruct((trows, width), bf),
        ),
        in_specs=[hbm, hbm, vmem, vmem],
        out_specs=(hbm, hbm),
        scratch_shapes=[
            pltpu.VMEM((heads, 3, rows, HD), bf),
            pltpu.VMEM((heads, 3, trows, HD), bf),
            pltpu.VMEM((2, nu, nb, 2, rows, HD), bf),
            pltpu.VMEM((nu, nb, 2, 2, trows, HD), bf),
            pltpu.VMEM((TILES, per, rows, HD), bf),
            pltpu.VMEM((TILES, per, trows, HD), bf),
            pltpu.VMEM((TILES, per, rows, HD), bf),
            pltpu.VMEM((TILES, per, trows, HD), bf),
            pltpu.VMEM((tile, HD), f32),
            pltpu.VMEM((TILES, tile, 2 * HD), bf),
            pltpu.VMEM((2, 2, nu * nb * trows, HD), bf),
            pltpu.VMEM((nu * nb * trows, HD), f32),
            pltpu.VMEM((TILES, tile, HD), f32),
            pltpu.VMEM((TILES, tile, 2 * HD), f32),
            pltpu.VMEM((tile, 2 * nu * rows), f32),
            pltpu.VMEM((tile, 2 * nu * rows), f32),
            dma((2,)), dma((2,)), dma((4,)),
            dma(()), dma(()), dma((2, nb)), dma(()), dma(()), dma(()), dma((TILES,)), dma(()), dma((TILES,)),
            dma((3,)), dma((2, nb)), dma((2, nb)), dma((2, nb)), dma((2, nb)), dma((2, nb)),
            dma(()), dma(()),
            dma(()), dma(()), dma(()), dma(()), dma((4,)),
        ],
        compiler_params=pltpu.CompilerParams(
            collective_id=0, has_side_effects=True, vmem_limit_bytes=60 * 1024 * 1024
        ),
        name="joint_attention",
    )(video_qkv, text_qkv, video_gate.reshape(heads, HD), text_gate.reshape(heads, HD))


def solution(mesh):
    in_specs = (
        P(None, ("req", "blk", "uly"), None),
        P(None, ("req", "blk", "uly"), None),
        P("req"),
        P("req"),
    )
    out_specs = (P(("req", "blk", "uly"), None), P(("req", "blk", "uly"), None))
    return jax.shard_map(
        on_device, mesh=mesh, in_specs=in_specs, out_specs=out_specs, check_vma=False
    )
```

```python
import functools
import math

import jax
import jax.numpy as jnp
from jax import lax
from jax.experimental import pallas as pl
from jax.experimental.pallas import tpu as pltpu
from jax.sharding import PartitionSpec as P

HD = 128
MESH = pl.DeviceIdType.MESH
TILES = 3
LAG = 4
DEPTH = 2 * LAG + 2


def near(j, n):
    if isinstance(j, int):
        return (j + 1) // 2 if j % 2 else (n - j // 2) % n
    return jnp.where(lax.rem(j, 2) == 1, (j + 1) // 2, lax.rem(n - j // 2, n))


def kernel(
    nb, nu, vid, txt, vgate, tgate, vout, tout,
    st, stt, kvb, txb, qb, qtb, ob, otb, qf, qq, ktx, tf, m_sc, acc_sc, s_a, s_b,
    l_st, l_kv, l_q, zs_kv, zs_r, zr_kv, zs_t, zr_t, zs_q, zr_q, zs_qt, zr_qt,
    xs, xl, xr, xf0, xf1, pc, ts, tr, os_, orv, ots, otr, ol,
):
    z = lax.axis_index("blk")
    u = lax.axis_index("uly")
    rows = vid.shape[1]
    trows = txt.shape[1]
    per = nb // 2
    up = u + 1 - 2 * lax.rem(u, 2)
    ul = lax.rem(u + nu - 2, nu)
    ur = lax.rem(u + 2, nu)
    uf = lax.rem(u + 4, nu)
    par = lax.rem(z, 2)

    barrier = pltpu.get_barrier_semaphore()
    for e in range(1, nb):
        pl.semaphore_signal(
            barrier, inc=1, device_id={"blk": lax.rem(z + e, nb)}, device_id_type=MESH
        )
    for e in range(1, nu):
        pl.semaphore_signal(
            barrier, inc=1, device_id={"uly": lax.rem(u + e, nu)}, device_id_type=MESH
        )

    def cols(h):
        return pl.ds(pl.multiple_of(h * HD, HD), HD)

    heads = st.shape[0]

    def stage(h, _):
        pltpu.make_async_copy(vid.at[:, :, cols(h)], st.at[h], l_st.at[0]).start()
        pltpu.make_async_copy(txt.at[:, :, cols(h)], stt.at[h], l_st.at[1]).start()
        return 0

    lax.fori_loop(0, heads, stage, 0)

    def low(t):
        return 3 * (t // 2) + lax.rem(t, 2)

    def own(t):
        return 3 * (t // 2) + 2 * lax.rem(t, 2)

    def shared(t):
        return 3 * (t // 2) + 1

    def shared_to(e):
        up_to = lax.rem(z + e, nb)
        return jnp.where(lax.rem(up_to, 2) == 0, up_to, lax.rem(z + nb - e, nb))

    def shared_back(e):
        return lax.rem(z + nb + (2 * par - 1) * e, nb)

    hs = low(z)
    for k, h in enumerate((own(z), shared(z))):
        pltpu.make_async_copy(
            vid.at[pl.ds(1, 2), :, cols(h)], kvb.at[k, u, 0], zr_kv.at[k, 0]
        ).start()
        pltpu.make_async_copy(
            txt.at[pl.ds(1, 2), :, cols(hs + k)], txb.at[u, 0, k], l_kv.at[k]
        ).start()
    for k, (s, h) in enumerate(((1, own(z)), (2, shared(z)))):
        pltpu.make_async_copy(vid.at[0, :, cols(h)], qb.at[s, per - 1], l_q.at[2 * k]).start()
        pltpu.make_async_copy(txt.at[0, :, cols(h)], qtb.at[s, per - 1], l_q.at[2 * k + 1]).start()

    pltpu.make_async_copy(st, st, l_st.at[0]).wait()
    pltpu.make_async_copy(stt, stt, l_st.at[1]).wait()
    pl.semaphore_wait(barrier, nb - 1 + nu - 1)

    def send(src, dst, ss, rs, dev):
        pltpu.make_async_remote_copy(
            src_ref=src, dst_ref=dst, send_sem=ss, recv_sem=rs, device_id=dev, device_id_type=MESH
        ).start()

    def send_queries(s):
        for i in range(per):
            if s < 2:
                d = near(nb - 1 - per * s - i, nb)
                t = lax.rem(z + nb - d, nb)
                h = own(t)
            else:
                d = per - 1 - i
                t = shared_to(d)
                h = shared(t)
            if d != 0:
                send(st.at[h, 0], qb.at[s, i], zs_q, zr_q.at[s], {"blk": t})
                send(stt.at[h, 0], qtb.at[s, i], zs_qt, zr_qt.at[s], {"blk": t})

    def send_own(j):
        d = near(j, nb)
        t = lax.rem(z + nb - d, nb)
        send(st.at[own(t), pl.ds(1, 2)], kvb.at[0, u, j], zs_kv, zr_kv.at[0, j], {"blk": t})

    send_queries(0)
    send_queries(1)
    for j in range(1, nb):
        d = near(j, nb)
        t = lax.rem(z + nb - d, nb)
        h = low(t)
        send(stt.at[pl.ds(h, 2), pl.ds(1, 2)], txb.at[u, d], zs_t, zr_t, {"blk": t})
    for e in range(1, per):
        t = shared_to(e)
        send(st.at[shared(t), pl.ds(1, 2)], kvb.at[1, u, e], zs_kv, zr_kv.at[1, e], {"blk": t})
    for j in range(1, per + 1):
        send_own(j)

    def piece_of(q):
        late = lax.rem(q, 2)
        slot = jnp.where(q < per, 1, jnp.where(q < 2 * per, 0, late))
        idx = jnp.where(q < per, q, jnp.where(q < 2 * per, q - per, q // 2))
        return slot, idx

    def arrived(ref, sem):
        pltpu.make_async_copy(ref, ref, sem).wait()

    right, left, partner = {"uly": ur}, {"uly": ul}, {"uly": up}

    def own_piece(q):
        k, i = piece_of(q)
        piece = kvb.at[k, u, i]
        arrived(piece, zr_kv.at[k, i])
        send(piece, piece, xs.at[0], xl.at[k, i], right)
        send(piece, piece, xs.at[1], xr.at[k, i], left)
        send(piece, piece, xs.at[2], pc.at[k, i], partner)

    def hand_on(e):
        send(kvb.at[1, u, e], kvb.at[1, u, per + e], zs_r, zr_kv.at[1, per + e], {"blk": z + 1 - 2 * par})

    def next_piece(q):
        k, i = piece_of(q)
        arrived(kvb.at[k, ul, i], xl.at[k, i])
        send(kvb.at[k, ul, i, 0], kvb.at[k, ul, i, 0], xs.at[0], xf0.at[k, i], right)
        send(kvb.at[k, ul, i], kvb.at[k, ul, i], xs.at[2], pc.at[k, i], partner)
        arrived(kvb.at[k, ur, i], xr.at[k, i])
        send(kvb.at[k, ur, i, 1], kvb.at[k, ur, i, 1], xs.at[1], xf1.at[k, i], left)
        send(kvb.at[k, ur, i], kvb.at[k, ur, i], xs.at[2], pc.at[k, i], partner)

    def far_piece(q):
        k, i = piece_of(q)
        arrived(kvb.at[k, uf, i, 0], xf0.at[k, i])
        send(kvb.at[k, uf, i, 0], kvb.at[k, uf, i, 0], xs.at[2], pc.at[k, i], partner)
        arrived(kvb.at[k, uf, i, 1], xf1.at[k, i])
        send(kvb.at[k, uf, i, 1], kvb.at[k, uf, i, 1], xs.at[2], pc.at[k, i], partner)

    scale = math.log2(math.e) / math.sqrt(HD)
    vrows = per * rows
    n_all = vrows + per * trows
    slots = (par, par, 1 - par)

    def scores_of(s, keys):
        kk = jnp.concatenate((keys, keys), axis=1)
        return lax.dot_general(
            qq[s], kk, (((1,), (1,)), ((), ())), preferred_element_type=jnp.float32
        )

    def soften(s, sref, values):
        scores = sref[...]
        old = m_sc[s]
        best = jnp.maximum(old, jnp.max(scores, axis=1, keepdims=True))
        m_sc[s] = best
        raised = jnp.exp2(scores - best[:, :1]).astype(jnp.bfloat16)
        factor = jnp.exp2(old - best)
        vv = jnp.concatenate((values, jnp.ones_like(values)), axis=1)
        product = jnp.dot(raised, vv, preferred_element_type=jnp.float32)
        acc_sc[s, :, :HD] = acc_sc[s, :, :HD] * factor + product[:, :HD]
        acc_sc[s, :, HD:] = acc_sc[s, :, HD:] * factor + product[:, HD:]

    bufs = (s_a, s_b)

    def step(block, n):
        for s in range(3):
            if s < 2:
                bufs[s % 2][:, :n] = scores_of(s, block(slots[s], 0))
            if s > 0:
                soften(s - 1, bufs[(s - 1) % 2].at[:, :n], block(slots[s - 1], 1))

    def prepare(s):
        remote = per
        if s > 0:
            arrived(qb.at[s, per - 1], l_q.at[2 * (s - 1)])
            arrived(qtb.at[s, per - 1], l_q.at[2 * (s - 1) + 1])
            remote = per - 1
        arrived(qb.at[s, pl.ds(0, remote)], zr_q.at[s])
        arrived(qtb.at[s, pl.ds(0, remote)], zr_qt.at[s])
        qf[0:vrows, :] = qb[s].astype(jnp.float32).reshape(vrows, HD)
        for i in range(per):
            at = vrows + i * trows
            qf[at : at + trows, :] = qtb[s, i].astype(jnp.float32)
        scaled = qf[...] * scale
        high = scaled.astype(jnp.bfloat16)
        qq[s, :, :HD] = high
        qq[s, :, HD:] = (scaled - high.astype(jnp.float32)).astype(jnp.bfloat16)

    def finish(s):
        h = own(z) if s < 2 else shared(z)
        attended = (acc_sc[s, :, :HD] / acc_sc[s, :, HD:]).astype(jnp.bfloat16).astype(jnp.float32)
        gated = attended[:vrows] * vgate[pl.ds(h, 1), :]
        ob[s] = gated.astype(jnp.bfloat16).reshape(per, rows, HD)
        tgated = attended[vrows:] * tgate[pl.ds(h, 1), :]
        for i in range(per):
            otb[s, i] = tgated[i * trows : (i + 1) * trows].astype(jnp.bfloat16)
        for i in range(per):
            if s < 2:
                d = near(nb - 1 - per * s - i, nb)
                t = lax.rem(z + d, nb)
            else:
                d = per - 1 - i
                t = shared_back(d)
            if d == 0:
                at = 2 * (s - 1)
                pltpu.make_async_copy(ob.at[s, i], vout.at[:, cols(h)], ol.at[at]).start()
                pltpu.make_async_copy(otb.at[s, i], tout.at[:, cols(h)], ol.at[at + 1]).start()
            else:
                send(ob.at[s, i], vout.at[:, cols(h)], os_, orv, {"blk": t})
                send(otb.at[s, i], tout.at[:, cols(h)], ots, otr, {"blk": t})

    def carry(q):
        @pl.when(q < 2 * nb)
        def _():
            own_piece(q)

        @pl.when(q < per)
        def _():
            hand_on(q)

        @pl.when((q >= 1) & (q < per))
        def _():
            send_own(per + q)

        @pl.when((q >= LAG) & (q < 2 * nb + LAG))
        def _():
            next_piece(q - LAG)

        @pl.when((q >= 2 * LAG) & (q < 2 * nb + 2 * LAG))
        def _():
            far_piece(q - 2 * LAG)

    def early(q, _):
        carry(q)
        return 0

    lax.fori_loop(0, per, early, 0)
    send_queries(2)

    for k in range(2):
        arrived(txb.at[u, 0, k], l_kv.at[k])
    arrived(txb.at[u, pl.ds(1, nb - 1)], zr_t)
    for e in range(1, nu):
        send(txb.at[u], txb.at[u], ts, tr, {"uly": lax.rem(u + e, nu)})
    m_sc[...] = jnp.full(m_sc.shape, -jnp.inf, jnp.float32)
    acc_sc[...] = jnp.zeros(acc_sc.shape, jnp.float32)
    prepare(0)
    prepare(1)
    lax.fori_loop(per, per + LAG, early, 0)

    arrived(txb.at[pl.ds(0, nu - 1)], tr)
    for k in range(2):
        for kv in range(2):
            for v in range(nu):
                for d in range(nb):
                    at = (v * nb + d) * trows
                    tf[at : at + trows, :] = txb[v, d, k, kv].astype(jnp.float32)
            ktx[k, kv] = tf[...].astype(jnp.bfloat16)
    step(lambda slot, kv: ktx[slot, kv], nu * nb * trows)

    quarter = kvb.at[0, pl.ds(0, nu // 2), 0]
    wide = 2 * nu * rows

    def keys_in(k, p):
        arrived(quarter, pc.at[k, 2 * p])
        arrived(quarter, pc.at[k, 2 * p + 1])

    def block(k, p, kv):
        return kvb[k, :, pl.ds(2 * p, 2), kv].reshape(wide, HD)

    def turn(q, _):
        carry(q)
        r = q - DEPTH
        place = lax.rem(r, 4)

        @pl.when(r == 2 * per)
        def _():
            prepare(2)

        @pl.when(((r > per) & (r < 2 * per) & (lax.rem(r, 2) == 1)) | ((r > 2 * per) & (place == 2)))
        def _():
            p = jnp.where(r < 2 * per, (r - per) // 2, r // 4)
            keys_in(0, p)
            step(lambda slot, kv: block(0, p, kv), wide)

        @pl.when((r >= 2 * per) & (place == 0))
        def _():
            p = r // 4 - per // 2
            keys_in(1, p)
            s_a[...] = scores_of(2, block(1, p, 0))
            soften(2, s_a, block(1, p, 1))

        return 0

    lax.fori_loop(per + LAG, 2 * nb + DEPTH - 1, turn, 0)
    finish(0)
    finish(1)

    n = nu * nb * trows
    bufs[0][:, :n] = scores_of(2, ktx[slots[2], 0])
    for i in range(per // 2):
        p = per // 2 + i
        keys_in(1, p)
        bufs[(i + 1) % 2][...] = scores_of(2, block(1, p, 0))
        if i == 0:
            soften(2, bufs[0].at[:, :n], ktx[slots[2], 1])
        else:
            soften(2, bufs[i % 2], block(1, p - 1, 1))
    soften(2, bufs[(per // 2) % 2], block(1, per - 1, 1))
    finish(2)

    for k in range(2):
        arrived(ob.at[0, 0], ol.at[2 * k])
        arrived(otb.at[0, 0], ol.at[2 * k + 1])
    n_out = nb - 1 + per - 1
    some = kvb.at[0, 0, pl.ds(0, n_out // 2)]
    small = txb.at[0, pl.ds(0, n_out // 2), 0]
    for sem in (os_, orv, zs_q):
        arrived(some, sem)
    for sem in (ots, otr, zs_qt):
        arrived(small, sem)
    arrived(kvb.at[0, pl.ds(0, 2), pl.ds(0, n_out // 2)], zs_kv)
    arrived(kvb.at[0, 0, pl.ds(0, per)], zs_r)
    arrived(txb.at[0, pl.ds(0, nb - 1)], zs_t)
    arrived(kvb.at[0, pl.ds(0, 3)], xs.at[0])
    arrived(kvb.at[0, pl.ds(0, 3)], xs.at[1])
    arrived(kvb.at[0], xs.at[2])
    arrived(txb.at[pl.ds(0, nu - 1)], ts)


def on_device(video_qkv, text_qkv, video_gate, text_gate):
    nb = lax.axis_size("blk")
    nu = lax.axis_size("uly")
    rows, width = video_qkv.shape[1:]
    trows = text_qkv.shape[1]
    heads = width // HD
    bf, f32 = jnp.bfloat16, jnp.float32
    per = nb // 2
    tile = per * (rows + trows)
    dma = pltpu.SemaphoreType.DMA
    hbm = pl.BlockSpec(memory_space=pl.ANY)
    vmem = pl.BlockSpec(memory_space=pltpu.VMEM)
    return pl.pallas_call(
        functools.partial(kernel, nb, nu),
        out_shape=(
            jax.ShapeDtypeStruct((rows, width), bf),
            jax.ShapeDtypeStruct((trows, width), bf),
        ),
        in_specs=[hbm, hbm, vmem, vmem],
        out_specs=(hbm, hbm),
        scratch_shapes=[
            pltpu.VMEM((heads, 3, rows, HD), bf),
            pltpu.VMEM((heads, 3, trows, HD), bf),
            pltpu.VMEM((2, nu, nb, 2, rows, HD), bf),
            pltpu.VMEM((nu, nb, 2, 2, trows, HD), bf),
            pltpu.VMEM((TILES, per, rows, HD), bf),
            pltpu.VMEM((TILES, per, trows, HD), bf),
            pltpu.VMEM((TILES, per, rows, HD), bf),
            pltpu.VMEM((TILES, per, trows, HD), bf),
            pltpu.VMEM((tile, HD), f32),
            pltpu.VMEM((TILES, tile, 2 * HD), bf),
            pltpu.VMEM((2, 2, nu * nb * trows, HD), bf),
            pltpu.VMEM((nu * nb * trows, HD), f32),
            pltpu.VMEM((TILES, tile, HD), f32),
            pltpu.VMEM((TILES, tile, 2 * HD), f32),
            pltpu.VMEM((tile, 2 * nu * rows), f32),
            pltpu.VMEM((tile, 2 * nu * rows), f32),
            dma((2,)), dma((2,)), dma((4,)),
            dma(()), dma(()), dma((2, nb)), dma(()), dma(()), dma(()), dma((TILES,)), dma(()), dma((TILES,)),
            dma((3,)), dma((2, nb)), dma((2, nb)), dma((2, nb)), dma((2, nb)), dma((2, nb)),
            dma(()), dma(()),
            dma(()), dma(()), dma(()), dma(()), dma((4,)),
        ],
        compiler_params=pltpu.CompilerParams(
            collective_id=0, has_side_effects=True, vmem_limit_bytes=60 * 1024 * 1024
        ),
        name="joint_attention",
    )(video_qkv, text_qkv, video_gate.reshape(heads, HD), text_gate.reshape(heads, HD))


def solution(mesh):
    in_specs = (
        P(None, ("req", "blk", "uly"), None),
        P(None, ("req", "blk", "uly"), None),
        P("req"),
        P("req"),
    )
    out_specs = (P(("req", "blk", "uly"), None), P(("req", "blk", "uly"), None))
    return jax.shard_map(
        on_device, mesh=mesh, in_specs=in_specs, out_specs=out_specs, check_vma=False
    )
```
